128 devices in a mesh: tm: 4 (over y), vox: 32 (over z, x, core).
Axes of the slice: x: 4, y: 4, z: 4, core: 2. Of those that a mesh axis runs over, the one named last changes fastest.
Arguments:
- frames: bfloat16 [4, 500, 524288], P('tm', None, 'vox'), as said below
- decay: float32 [4, 500], P('tm'), may hold values from 0.3 to 1
- start: float32 [500, 64], replicated, may hold values from -6 to 6
- clutter_cut: int32 [4], P('tm'), may hold values from 8 to 15
- noise_cut: int32 [4], P('tm'), may hold values from 32 to 63
Outputs:
- power: float32 [4, 524288], P('tm', 'vox')
The draws below stay inside these ranges and needn't reach their ends.
Inputs may be any that keep to these rules, and one draw needn't show every extreme that they name: `frames`: each window is a sum of temporal patterns times voxel maps, plus independent noise.
All inputs are finite; a program needn't handle non-finite values.
Results may differ from the reference program's by a relative error of at most 0.00045.
Values sent between devices are 32-bit elements; how exact they have to be, the bound alone decides.
No kernel may reach another device: no remote copies, remote signals or barrier semaphores. Data moves between devices by JAX's collectives and lax.ppermute only.
A program may use at most 128 MiB of HBM per device.

```python
import math
import jax
import jax.numpy as jnp
from jax import lax

W = 500
RANK = 64
ITERS = 6
VOX_DEV = 16384
VOXELS = 524288
STEPS = 4


def draw_frames(key, part):
    comps = 2 * RANK + RANK // 2
    block_count = VOXELS // VOX_DEV
    shared = jax.random.normal(jax.random.fold_in(key, 11), (W, comps), jnp.float32)
    order = jnp.arange(comps, dtype=jnp.float32)
    strength = 10.0 * 0.97 ** order * jnp.where(order < RANK // 4, 3.0, 1.0)
    block_level = jnp.exp(jax.random.uniform(jax.random.fold_in(key, 13), (comps, block_count), jnp.float32, math.log(0.2), math.log(5.0)))

    def one_step(step_index):
        step_key = jax.random.fold_in(key, step_index)
        drift = jax.random.normal(jax.random.fold_in(step_key, 1), (W, comps), jnp.float32)
        temporal = (shared + 0.3 * drift) / math.sqrt(W) * strength[None, :]
        frame_level = jnp.exp(jax.random.uniform(jax.random.fold_in(step_key, 4), (W,), jnp.float32, math.log(0.3), math.log(3.0)))
        spatial = jax.random.normal(jax.random.fold_in(step_key, 2), (comps, block_count, VOX_DEV), jnp.float32)
        spatial = (spatial * block_level[:, :, None]).reshape(comps, VOXELS)
        noise = jax.random.normal(jax.random.fold_in(step_key, 3), (W, VOXELS), jnp.float32)
        signal = jnp.dot(temporal, spatial) + 0.5 * frame_level[:, None] * noise
        return signal.astype(jnp.bfloat16)
    return lax.map(one_step, jnp.arange(STEPS, dtype=jnp.int32))


def touch_ends(entries, key, least, high):
    shape = entries.shape
    index_at = [jax.random.randint(jax.random.fold_in(key, axis), (), 0, shape[axis]) for axis in range(len(shape))]
    entries = entries.at[tuple(index_at)].set(least)
    longest = shape.index(max(shape))
    index_at[longest] = (index_at[longest] + 1) % shape[longest]
    return entries.at[tuple(index_at)].set(high)


def block_levels(own_key, dims, cuts, smallest, top_value):
    def one(dim, blocks):
        heights = jax.random.uniform(jax.random.fold_in(jax.random.fold_in(own_key, 6), dim), (blocks,), jnp.float32, smallest / len(cuts), top_value / len(cuts))
        return jnp.repeat(jnp.exp(heights), dims[dim] // blocks).reshape((-1,) + (1,) * (len(dims) - dim - 1))

    loudness = one(*cuts[0])
    for cut in cuts[1:]:
        loudness = loudness * one(*cut)
    return loudness


def centred(key, dims, scale, reach, kind=jnp.bfloat16):
    result = scale * jax.random.normal(key, dims, jnp.float32)
    return jnp.clip(result, min=-reach, max=reach).astype(kind)


def setup_inputs(seed: int = 0) -> dict:
    keys = jax.random.split(jax.random.key(seed), 6)
    return {
        "frames": draw_frames(jax.random.fold_in(keys[5], 71), 0),
        "decay": jnp.clip(jnp.exp(math.log(1.0) - 1.2039728 * jax.random.uniform(keys[1], (STEPS, W), jnp.float32) ** block_levels(keys[1], (STEPS, W), ((0, 4),), -0.2, 0.2)), 0.3, 1.0),
        "start": centred(keys[2], (W, RANK), 1.0, 6.0, jnp.float32),
        "clutter_cut": touch_ends(jax.random.randint(keys[3], (STEPS,), RANK // 8, RANK // 4), jax.random.fold_in(keys[3], 1), RANK // 8, (RANK // 4) - 1).astype(jnp.int32),
        "noise_cut": touch_ends(jax.random.randint(keys[4], (STEPS,), RANK // 2, RANK), jax.random.fold_in(keys[4], 1), RANK // 2, RANK - 1).astype(jnp.int32),
    }


def orthonormal(product):
    highest = lax.Precision.HIGHEST
    for sweep_index in range(2):
        cross_gram = jnp.dot(product.T, product, precision=highest)
        factor = jnp.linalg.cholesky(cross_gram)
        product = lax.linalg.triangular_solve(factor, product, left_side=False, lower=True, transpose_a=True)
    return product

def reference(frames, decay, start, clutter_cut, noise_cut):
    highest = lax.Precision.HIGHEST
    frame_count = frames.shape[1]
    weighted = jnp.zeros((frame_count, frame_count), jnp.float32)
    component = jnp.arange(RANK, dtype=jnp.int32)
    powers = []
    for step_index in range(STEPS):
        window = frames[step_index]
        gram_part = lax.dot_general(window.astype(jnp.float32), window.astype(jnp.float32), (((1,), (1,)), ((), ())), preferred_element_type=jnp.float32)
        forget = decay[step_index]
        weighted = forget[:, None] * forget[None, :] * weighted + gram_part
        subspace = start
        for sweep_index in range(ITERS):
            subspace = orthonormal(jnp.dot(weighted, subspace, precision=highest))
        subspace_low = subspace.astype(jnp.bfloat16)
        project = lax.dot_general(subspace_low.astype(jnp.float32), window.astype(jnp.float32), (((0,), (0,)), ((), ())), preferred_element_type=jnp.float32)
        passband = ((component >= clutter_cut[step_index]) & (component < noise_cut[step_index])).astype(jnp.float32)
        powers.append(jnp.sum(passband[:, None] * project * project, axis=0) / frame_count)
    return jnp.stack(powers)
```

```python
import functools

import jax
import jax.numpy as jnp
from jax import lax
from jax.experimental import pallas as pl
from jax.experimental.pallas import tpu as pltpu
from jax.sharding import PartitionSpec as P

ITERS = 6
CHUNK = 2048
COLS = 1024


def chunk_copy(frames_ref, kept_ref, sems, turn):
    span = pl.ds(turn * CHUNK, CHUNK)
    return pltpu.make_async_copy(frames_ref.at[0, :, span], kept_ref.at[:, span], sems.at[turn])


def gram_kernel(chunks, frames_ref, packed_ref, kept_ref, top_ref, cross_ref, low_ref, sems):
    copy = functools.partial(chunk_copy, frames_ref, kept_ref, sems)

    for turn in range(chunks):
        copy(turn).start()
    top_ref[...] = jnp.zeros_like(top_ref)
    cross_ref[...] = jnp.zeros_like(cross_ref)
    low_ref[...] = jnp.zeros_like(low_ref)
    rows = kept_ref.shape[0]
    rest = rows - 256

    def product(a, b):
        return lax.dot_general(a, b, (((1,), (1,)), ((), ())), preferred_element_type=jnp.float32)

    def one(turn, carry):
        copy(turn).wait()
        span = pl.ds(pl.multiple_of(turn * CHUNK, CHUNK), CHUNK)
        upper = kept_ref[0:256, span]
        lower = kept_ref[256:rows, span]
        top_ref[...] += product(upper, upper)
        cross_ref[0:rest, :] += product(lower, upper)
        low_ref[0:rest, 0:rest] += product(lower, lower)
        return carry

    lax.fori_loop(0, chunks, one, 0)
    down = lax.broadcasted_iota(jnp.int32, (256, 256), 0)
    across = lax.broadcasted_iota(jnp.int32, (256, 256), 1)
    low = low_ref[...]
    folded = jnp.where(down >= across, top_ref[...], low)
    diagonal = jnp.sum(jnp.where(down == across, low, 0.0), axis=0, keepdims=True)
    cross = jnp.where(down == 255, jnp.broadcast_to(diagonal, (256, 256)), cross_ref[...])
    packed_ref[0:256, :] = folded[:, :128]
    packed_ref[256:512, :] = cross[:, :128]
    packed_ref[512:768, :] = folded[:, 128:]
    packed_ref[768:1024, :] = cross[:, 128:]


def local_gram(frames):
    rows, columns = frames.shape[1:]
    chunks = columns // CHUNK
    return pl.pallas_call(
        functools.partial(gram_kernel, chunks),
        out_shape=jax.ShapeDtypeStruct((1024, 128), jnp.float32),
        in_specs=[pl.BlockSpec(memory_space=pltpu.HBM)],
        out_specs=pl.BlockSpec(memory_space=pltpu.VMEM),
        scratch_shapes=[
            pltpu.VMEM((rows, columns), frames.dtype),
            pltpu.VMEM((256, 256), jnp.float32),
            pltpu.VMEM((256, 256), jnp.float32),
            pltpu.VMEM((256, 256), jnp.float32),
            pltpu.SemaphoreType.DMA((chunks,)),
        ],
        compiler_params=pltpu.CompilerParams(vmem_limit_bytes=56 * 2**20),
        cost_estimate=pl.CostEstimate(
            flops=2 * rows * rows * columns, bytes_accessed=2 * rows * columns, transcendentals=0
        ),
        name="local_gram",
    )(frames)


def chain_kernel(steps, group, parts_ref, rates_ref, out_ref):
    held = None
    for step in range(steps):
        part = jnp.sum(parts_ref[step * group : (step + 1) * group], axis=0)
        held = part if step == 0 else rates_ref[step] * held + part
        out_ref[step * group : (step + 1) * group] = jnp.broadcast_to(held[None], (group, 8, 128))


def chain(parts, rates):
    steps = rates.shape[0]
    return pl.pallas_call(
        functools.partial(chain_kernel, steps, parts.shape[0] // steps),
        out_shape=jax.ShapeDtypeStruct(parts.shape, parts.dtype),
        compiler_params=pltpu.CompilerParams(vmem_limit_bytes=4 * 2**20),
        name="chain",
    )(parts, rates)


def split(x):
    high = x.astype(jnp.bfloat16)
    rest = x - high.astype(jnp.float32)
    middle = rest.astype(jnp.bfloat16)
    return high, middle, (rest - middle.astype(jnp.float32)).astype(jnp.bfloat16)


def mul(a, b, along=0):
    return lax.dot_general(
        a, b, (((1,), (along,)), ((), ())), preferred_element_type=jnp.float32
    )


def full_product(left, right, along=0):
    size = left[0].shape[0]
    stacked = jnp.concatenate(left, axis=0)
    first = mul(stacked, right[0], along)
    second = mul(stacked[: 2 * size], right[1], along)
    third = mul(left[0], right[2], along)
    small = first[2 * size :] + second[size:] + third
    return first[:size] + (first[size : 2 * size] + second[:size] + small)


def spread(x, index):
    return jnp.broadcast_to(x[index : index + 1, :], x.shape)


def eliminated(rows):
    rows = list(rows)
    count = len(rows)
    sub = lax.broadcasted_iota(jnp.int32, (8, 128), 0)
    scales = []
    for block in range(count):
        columns = {
            v: [
                jnp.broadcast_to(rows[v][:, 8 * block + k : 8 * block + k + 1], (8, 128))
                for k in range(8)
            ]
            for v in range(block, count)
        }
        pivots = jnp.ones((8, 128), jnp.float32)
        for j in range(8):
            pivot = spread(columns[block][j], j)
            pivots = jnp.where(sub == j, pivot, pivots)
            inverse = 1.0 / pivot
            row = spread(rows[block], j) * inverse
            parts = {k: spread(columns[block][k], j) * inverse for k in range(j + 1, 8)}
            for v in range(block, count):
                lead = columns[v][j]
                if v == block:
                    lead = jnp.where(sub > j, lead, 0.0)
                for k in range(j + 1, 8):
                    columns[v][k] = columns[v][k] - lead * parts[k]
                rows[v] = rows[v] - lead * row
        scales.append(lax.rsqrt(pivots))
    return [r * s for r, s in zip(rows, scales)]


def power_kernel(
    chunks, packed_ref, start_ref, low_ref, high_ref, frames_ref, out_ref,
    a1_ref, a2_ref, a3_ref, kept_ref, sems,
):
    copy = functools.partial(chunk_copy, frames_ref, kept_ref, sems)
    for turn in range(chunks):
        copy(turn).start()
    down = lax.broadcasted_iota(jnp.int32, (256, 256), 0)
    across = lax.broadcasted_iota(jnp.int32, (256, 256), 1)
    folded = jnp.concatenate([packed_ref[0:256, :], packed_ref[512:768, :]], axis=1)
    cross = jnp.concatenate([packed_ref[256:512, :], packed_ref[768:1024, :]], axis=1)
    turned = folded.T
    top = jnp.where(down >= across, folded, turned)
    low = jnp.where(down < across, folded, turned)
    low = jnp.where(down == across, jnp.broadcast_to(cross[255:256, :], (256, 256)), low)
    cross = jnp.where(down == 255, 0.0, cross)

    def put(piece, i, j):
        for ref, part in zip((a1_ref, a2_ref, a3_ref), split(piece)):
            ref[256 * i : 256 * (i + 1), 256 * j : 256 * (j + 1)] = part

    put(top, 0, 0)
    put(low, 1, 1)
    put(cross, 1, 0)
    put(cross.T, 0, 1)

    rank, frames = start_ref.shape
    beside = lax.broadcasted_iota(jnp.int32, (rank, 128), 0) + rank
    unit = jnp.where(
        lax.broadcasted_iota(jnp.int32, (rank, 128), 1) == beside, 1.0, 0.0
    ).astype(jnp.float32)
    none = jnp.zeros((rank, frames), jnp.bfloat16)

    def sweep(turn, product):
        parts = split(product)
        right = [jnp.concatenate([p, none], axis=0) for p in parts]
        grown = full_product(parts, right, 1) + unit
        rows = eliminated([grown[8 * v : 8 * (v + 1), :] for v in range(rank // 8)])
        factor = jnp.concatenate(rows, axis=0)
        return full_product(split(factor), [jnp.concatenate([none, p], axis=0) for p in parts])

    def iteration(turn, subspace):
        product = full_product(split(subspace), (a1_ref[...], a2_ref[...], a3_ref[...]))
        return lax.fori_loop(0, 2, sweep, product)

    subspace = lax.fori_loop(0, ITERS, iteration, start_ref[...])
    rows = kept_ref.shape[0]
    subspace_low = subspace.astype(jnp.bfloat16)[:, :rows]
    component = lax.broadcasted_iota(jnp.int32, (rank, COLS), 0)
    band = (component >= low_ref[0]) & (component < high_ref[0])

    def arrive(turn, carry):
        copy(turn).wait()
        return carry

    lax.fori_loop(0, chunks, arrive, 0)

    def project(turn, carry):
        span = pl.ds(pl.multiple_of(turn * COLS, COLS), COLS)
        values = mul(subspace_low, kept_ref[:, span])
        values = jnp.where(band, values, 0.0)
        out_ref[:, span] = jnp.sum(values * values, axis=0, keepdims=True) / rows
        return carry

    lax.fori_loop(0, kept_ref.shape[1] // COLS, project, 0)


def power_of(packed, start, low, high, frames):
    rows, columns = frames.shape[1:]
    chunks = columns // CHUNK
    return pl.pallas_call(
        functools.partial(power_kernel, chunks),
        out_shape=jax.ShapeDtypeStruct((1, columns), jnp.float32),
        in_specs=[
            pl.BlockSpec(memory_space=pltpu.VMEM),
            pl.BlockSpec(memory_space=pltpu.VMEM),
            pl.BlockSpec(memory_space=pltpu.SMEM),
            pl.BlockSpec(memory_space=pltpu.SMEM),
            pl.BlockSpec(memory_space=pltpu.HBM),
        ],
        out_specs=pl.BlockSpec(memory_space=pltpu.VMEM),
        scratch_shapes=[pltpu.VMEM((512, 512), jnp.bfloat16)] * 3
        + [pltpu.VMEM((rows, columns), frames.dtype), pltpu.SemaphoreType.DMA((chunks,))],
        compiler_params=pltpu.CompilerParams(vmem_limit_bytes=56 * 2**20),
        name="power",
    )(packed, start, low, high, frames)


def tile_rates(decay):
    steps, group = lax.axis_size("tm"), lax.axis_size("vox")
    step = lax.axis_index("tm")
    turns = [decay] + [
        lax.ppermute(decay, "tm", [(i, (i + k) % steps) for i in range(steps)])
        for k in range(1, steps)
    ]
    every = []
    for t in range(steps):
        mine = jnp.zeros_like(decay)
        for k in range(steps):
            mine = mine + jnp.where((step - t) % steps == k, turns[k], 0.0)
        every.append(mine)
    rates = jnp.stack(every)
    rates = jnp.pad(rates, ((0, 0), (0, 512 - rates.shape[1])))
    tile = step * group + lax.axis_index("vox")
    first_row = 8 * (tile % 64)
    first_column = 128 * (tile // 64)
    row = first_row + lax.broadcasted_iota(jnp.int32, (8, 128), 0)
    column = first_column + lax.broadcasted_iota(jnp.int32, (8, 128), 1)

    def at_rows(first):
        return lax.dynamic_slice_in_dim(rates, first, 8, 1)[:, :, None]

    def at_columns(first):
        return lax.dynamic_slice_in_dim(rates, first, 128, 1)[:, None, :]

    upper = at_rows(first_row) * at_columns(first_column)
    last = at_columns(256 + first_column)
    lower = at_rows(jnp.minimum(256 + first_row, 504)) * last
    return jnp.where(
        row == 511,
        last * last,
        jnp.where((row >= 256) | (row >= column), upper, lower),
    )


def per_device(frames, decay, start, clutter_cut, noise_cut):
    rates = tile_rates(decay[0])
    packed = local_gram(frames)
    parts = lax.all_to_all(packed.reshape(128, 8, 128), ("tm", "vox"), 0, 0, tiled=True)
    held = lax.all_to_all(chain(parts, rates), ("tm", "vox"), 0, 0, tiled=True)
    begin = jnp.pad(start.T, ((0, 0), (0, 512 - start.shape[0])))
    return power_of(held.reshape(1024, 128), begin, clutter_cut, noise_cut, frames)


def solution(mesh):
    placed = (P("tm", None, "vox"), P("tm", None), P(), P("tm"), P("tm"))
    return jax.shard_map(
        per_device, mesh=mesh, in_specs=placed, out_specs=P("tm", "vox"), check_vma=False
    )
```

```python
import functools

import jax
import jax.numpy as jnp
from jax import lax
from jax.experimental import pallas as pl
from jax.experimental.pallas import tpu as pltpu
from jax.sharding import Mesh, PartitionSpec as P


ITERS = 6
CHUNK = 2048
COLS = 4096


def chunk_copy(frames_ref, kept_ref, sems, turn):
    span = pl.ds(turn * CHUNK, CHUNK)
    return pltpu.make_async_copy(frames_ref.at[0, :, span], kept_ref.at[:, span], sems.at[turn])


def gram_kernel(chunks, core_ref, frames_ref, own_ref, other_ref, kept_ref, top_ref, cross_ref, low_ref, sems):
    copy = functools.partial(chunk_copy, frames_ref, kept_ref, sems)

    for turn in range(chunks):
        copy(turn).start()
    top_ref[...] = jnp.zeros_like(top_ref)
    cross_ref[...] = jnp.zeros_like(cross_ref)
    low_ref[...] = jnp.zeros_like(low_ref)
    rows = kept_ref.shape[0]
    rest = rows - 256

    def product(a, b):
        return lax.dot_general(a, b, (((1,), (1,)), ((), ())), preferred_element_type=jnp.float32)

    def one(turn, carry):
        copy(turn).wait()
        span = pl.ds(pl.multiple_of(turn * CHUNK, CHUNK), CHUNK)
        upper = kept_ref[0:256, span]
        lower = kept_ref[256:rows, span]
        top_ref[...] += product(upper, upper)
        cross_ref[0:rest, :] += product(lower, upper)
        low_ref[0:rest, 0:rest] += product(lower, lower)
        return carry

    lax.fori_loop(0, chunks, one, 0)
    down = lax.broadcasted_iota(jnp.int32, (256, 256), 0)
    across = lax.broadcasted_iota(jnp.int32, (256, 256), 1)
    low = low_ref[...]
    folded = jnp.where(down >= across, top_ref[...], low)
    diagonal = jnp.sum(jnp.where(down == across, low, 0.0), axis=0, keepdims=True)
    cross = jnp.where(down == 255, jnp.broadcast_to(diagonal, (256, 256)), cross_ref[...])
    first = core_ref[0] == 0
    for spot, piece in ((0, folded), (256, cross)):
        left, right = piece[:, :128], piece[:, 128:]
        own_ref[spot : spot + 256, :] = jnp.where(first, left, right)
        other_ref[spot : spot + 256, :] = jnp.where(first, right, left)


def local_gram(core, frames):
    rows, columns = frames.shape[1:]
    chunks = columns // CHUNK
    return pl.pallas_call(
        functools.partial(gram_kernel, chunks),
        out_shape=[pltpu.VMEM((512, 128), jnp.float32)] * 2,
        in_specs=[pl.BlockSpec(memory_space=pltpu.SMEM), pl.BlockSpec(memory_space=pltpu.HBM)],
        out_specs=[pl.BlockSpec(memory_space=pltpu.VMEM)] * 2,
        scratch_shapes=[
            pltpu.VMEM((rows, columns), frames.dtype),
            pltpu.VMEM((256, 256), jnp.float32),
            pltpu.VMEM((256, 256), jnp.float32),
            pltpu.VMEM((256, 256), jnp.float32),
            pltpu.SemaphoreType.DMA((chunks,)),
        ],
        compiler_params=pltpu.CompilerParams(vmem_limit_bytes=56 * 2**20),
        cost_estimate=pl.CostEstimate(
            flops=2 * rows * rows * columns, bytes_accessed=2 * rows * columns, transcendentals=0
        ),
        name="local_gram",
    )(core, frames)


def chain_kernel(steps, group, parts_ref, rates_ref, out_ref):
    held = None
    for step in range(steps):
        part = jnp.sum(parts_ref[step * group : (step + 1) * group], axis=0)
        held = part if step == 0 else rates_ref[step] * held + part
        out_ref[step * group : (step + 1) * group] = jnp.broadcast_to(held[None], (group, 8, 128))


def chain(parts, rates):
    steps = rates.shape[0]
    return pl.pallas_call(
        functools.partial(chain_kernel, steps, parts.shape[0] // steps),
        out_shape=jax.ShapeDtypeStruct(parts.shape, parts.dtype),
        compiler_params=pltpu.CompilerParams(vmem_limit_bytes=4 * 2**20),
        name="chain",
    )(parts, rates)


def split(x):
    high = x.astype(jnp.bfloat16)
    rest = x - high.astype(jnp.float32)
    middle = rest.astype(jnp.bfloat16)
    return high, middle, (rest - middle.astype(jnp.float32)).astype(jnp.bfloat16)


def mul(a, b, along=0):
    return lax.dot_general(
        a, b, (((1,), (along,)), ((), ())), preferred_element_type=jnp.float32
    )


def full_product(left, right, along=0):
    size = left[0].shape[0]
    stacked = jnp.concatenate(left, axis=0)
    first = mul(stacked, right[0], along)
    second = mul(stacked[: 2 * size], right[1], along)
    third = mul(left[0], right[2], along)
    small = first[2 * size :] + second[size:] + third
    return first[:size] + (first[size : 2 * size] + second[:size] + small)


def spread(x, index):
    return jnp.broadcast_to(x[index : index + 1, :], x.shape)


def eliminated(rows, none):
    rows = list(rows)
    count = len(rows)
    sub = lax.broadcasted_iota(jnp.int32, (8, 128), 0)

    def columns_of(v, first, size):
        return [
            jnp.broadcast_to(rows[v][:, first + k : first + k + 1], (8, 128))
            for k in range(size)
        ]

    done = []
    for a in range(0, count, 2):
        b = a + 1
        top = [column + none for column in columns_of(a, 8 * a, 8)]
        side = [column + none for column in columns_of(b, 8 * a, 8)]
        low = columns_of(b, 8 * b, 8)
        rest = {v: columns_of(v, 8 * a, 16) for v in range(b + 1, min(b + 3, count))}
        scales = []
        for half, own in ((0, top), (1, low)):
            pivots = jnp.ones((8, 128), jnp.float32)
            pivot = spread(own[0], 0)
            for j in range(8):
                pivots = jnp.where(sub == j, pivot, pivots)
                inverse = 1.0 / pivot
                heads = [spread(own[k], j) if k > j else None for k in range(8)]
                if j < 7:
                    pivot = spread(own[j + 1], j + 1) - (
                        spread(own[j], j + 1) * inverse
                    ) * heads[j + 1]
                lead = jnp.where(sub > j, own[j], 0.0) * inverse
                row = spread(rows[a + half], j)
                if half == 0:
                    beside = side[j] * inverse
                    others = [spread(side[j], k) for k in range(8)]
                    rows[b] = rows[b] - beside * row
                    for k in range(8):
                        low[k] = low[k] - beside * others[k]
                rows[a + half] = rows[a + half] - lead * row
                for k in range(j + 1, 8):
                    own[k] = own[k] - lead * heads[k]
                    if half == 0:
                        side[k] = side[k] - beside * heads[k]
                for v, held in rest.items():
                    far = held[8 * half + j] * inverse
                    for k in range(j + 1, 8):
                        held[8 * half + k] = held[8 * half + k] - far * heads[k]
                    if half == 0:
                        for k in range(8):
                            held[8 + k] = held[8 + k] - far * others[k]
                    rows[v] = rows[v] - far * row
            scales.append(1.0 / pivots)
            done.append(lax.rsqrt(pivots))
        if b + 3 < count:
            u1, u2, u3 = split(jnp.concatenate([rows[a], rows[b]], axis=0))
            t1, t2, t3 = split(
                jnp.concatenate([rows[a] * scales[0], rows[b] * scales[1]], axis=0)
            )
            change = lax.dot_general(
                jnp.concatenate([u1, u1, u2, u2, u1, u3], axis=0)[:, : 8 * count],
                jnp.concatenate([t1, t2, t1, t2, t3, t1], axis=0),
                (((0,), (0,)), ((), ())),
                preferred_element_type=jnp.float32,
            )
            for v in range(b + 3, count):
                rows[v] = rows[v] - change[8 * v : 8 * (v + 1), :]
    return [r * s for r, s in zip(rows, done)]


def power_kernel(
    chunks, core_ref, own_ref, other_ref, start_ref, low_ref, high_ref, frames_ref, out_ref,
    a1_ref, a2_ref, a3_ref, sized_ref, second_ref, kept_ref, zero_ref, sems,
):
    copy = functools.partial(chunk_copy, frames_ref, kept_ref, sems)
    for turn in range(chunks):
        copy(turn).start()
    zero_ref[...] = jnp.zeros_like(zero_ref)
    down = lax.broadcasted_iota(jnp.int32, (256, 256), 0)
    across = lax.broadcasted_iota(jnp.int32, (256, 256), 1)
    first = core_ref[0] == 0

    def whole(spot):
        own, other = own_ref[spot : spot + 256, :], other_ref[spot : spot + 256, :]
        return jnp.concatenate(
            [jnp.where(first, own, other), jnp.where(first, other, own)], axis=1
        )

    folded, cross = whole(0), whole(256)
    turned = folded.T
    top = jnp.where(down >= across, folded, turned)
    low = jnp.where(down < across, folded, turned)
    low = jnp.where(down == across, jnp.broadcast_to(cross[255:256, :], (256, 256)), low)
    cross = jnp.where(down == 255, 0.0, cross)

    def put(piece, i, j):
        for ref, part in zip((a1_ref, a2_ref, a3_ref), split(piece)):
            ref[256 * i : 256 * (i + 1), 256 * j : 256 * (j + 1)] = part

    put(top, 0, 0)
    put(low, 1, 1)
    put(cross, 1, 0)
    put(cross.T, 0, 1)

    rank, frames = start_ref.shape
    beside = lax.broadcasted_iota(jnp.int32, (rank, 128), 0) + rank
    unit = jnp.where(
        lax.broadcasted_iota(jnp.int32, (rank, 128), 1) == beside, 1.0, 0.0
    ).astype(jnp.float32)
    none = jnp.zeros((rank, frames), jnp.bfloat16)

    def under(parts):
        return [jnp.concatenate([none[:, : p.shape[1]], p], axis=0) for p in parts]

    def over(parts):
        return [jnp.concatenate([p, none[:, : p.shape[1]]], axis=0) for p in parts]

    def factor_of(gram):
        grown = gram + unit
        tiles = [grown[8 * v : 8 * (v + 1), :] for v in range(rank // 8)]
        return split(jnp.concatenate(eliminated(tiles, zero_ref[...]), axis=0))

    weights = (a1_ref, a2_ref, a3_ref)

    def iteration(turn, carry):
        product, gram = carry
        sized = split(full_product(factor_of(gram), under(split(product))))
        second = factor_of(full_product(sized, over(sized), 1))
        for at, part in enumerate(sized):
            sized_ref[at] = part
        for at, part in enumerate(second):
            second_ref[at] = part
        ahead = split(full_product(sized, [w[...] for w in weights]))
        square = split(full_product(ahead, under(ahead), 1))
        product = full_product(second, under(ahead))
        half = full_product(second, under(square))
        return product, full_product(split(half), over(second), 1)

    product = full_product(split(start_ref[...]), [w[...] for w in weights])
    parts = split(product)
    lax.fori_loop(0, ITERS, iteration, (product, full_product(parts, over(parts), 1)))
    subspace = full_product(
        [second_ref[at] for at in range(3)], under([sized_ref[at] for at in range(3)])
    )
    rows = kept_ref.shape[0]
    subspace_low = subspace.astype(jnp.bfloat16)[:, :rows]
    component = lax.broadcasted_iota(jnp.int32, (rank, COLS), 0)
    band = (component >= low_ref[0]) & (component < high_ref[0])

    def arrive(turn, carry):
        copy(turn).wait()
        return carry

    lax.fori_loop(0, chunks, arrive, 0)

    def project(turn, carry):
        span = pl.ds(pl.multiple_of(turn * COLS, COLS), COLS)
        values = mul(subspace_low, kept_ref[:, span])
        values = jnp.where(band, values, 0.0)
        out_ref[:, span] = jnp.sum(values * values, axis=0, keepdims=True) / rows
        return carry

    lax.fori_loop(0, kept_ref.shape[1] // COLS, project, 0)


def power_of(core, own, other, start, low, high, frames):
    rows, columns = frames.shape[1:]
    chunks = columns // CHUNK
    return pl.pallas_call(
        functools.partial(power_kernel, chunks),
        out_shape=jax.ShapeDtypeStruct((1, columns), jnp.float32),
        in_specs=[
            pl.BlockSpec(memory_space=pltpu.SMEM),
            pl.BlockSpec(memory_space=pltpu.VMEM),
            pl.BlockSpec(memory_space=pltpu.VMEM),
            pl.BlockSpec(memory_space=pltpu.VMEM),
            pl.BlockSpec(memory_space=pltpu.SMEM),
            pl.BlockSpec(memory_space=pltpu.SMEM),
            pl.BlockSpec(memory_space=pltpu.HBM),
        ],
        out_specs=pl.BlockSpec(memory_space=pltpu.VMEM),
        scratch_shapes=[pltpu.VMEM((512, 512), jnp.bfloat16)] * 3
        + [
            pltpu.VMEM((3, 64, 512), jnp.bfloat16),
            pltpu.VMEM((3, 64, 128), jnp.bfloat16),
            pltpu.VMEM((rows, columns), frames.dtype),
            pltpu.VMEM((8, 128), jnp.float32),
            pltpu.SemaphoreType.DMA((chunks,)),
        ],
        compiler_params=pltpu.CompilerParams(vmem_limit_bytes=40 * 2**20),
        name="power",
    )(core, own, other, start, low, high, frames)


def tile_rates(decay):
    steps, group = lax.axis_size("tm"), lax.axis_size("chip")
    step = lax.axis_index("tm")
    turns = [decay] + [
        lax.ppermute(decay, "tm", [(i, (i + k) % steps) for i in range(steps)])
        for k in range(1, steps)
    ]
    every = []
    for t in range(steps):
        mine = jnp.zeros_like(decay)
        for k in range(steps):
            mine = mine + jnp.where((step - t) % steps == k, turns[k], 0.0)
        every.append(mine)
    rates = jnp.stack(every)
    rates = jnp.pad(rates, ((0, 0), (0, 512 - rates.shape[1])))
    first_row = 8 * (step * group + lax.axis_index("chip"))
    first_column = 128 * lax.axis_index("core")
    row = first_row + lax.broadcasted_iota(jnp.int32, (8, 128), 0)
    column = first_column + lax.broadcasted_iota(jnp.int32, (8, 128), 1)

    def at_rows(first):
        return lax.dynamic_slice_in_dim(rates, first, 8, 1)[:, :, None]

    def at_columns(first):
        return lax.dynamic_slice_in_dim(rates, first, 128, 1)[:, None, :]

    upper = at_rows(first_row) * at_columns(first_column)
    last = at_columns(256 + first_column)
    lower = at_rows(jnp.minimum(256 + first_row, 504)) * last
    return jnp.where(
        row == 511,
        last * last,
        jnp.where((row >= 256) | (row >= column), upper, lower),
    )


def swapped(x):
    return lax.ppermute(x, "core", [(0, 1), (1, 0)])


def exchanged(tiles):
    return lax.all_to_all(tiles, ("tm", "chip"), 0, 0, tiled=True)


def per_device(frames, decay, start, clutter_cut, noise_cut):
    core = lax.axis_index("core").reshape(1)
    rates = tile_rates(decay[0])
    own, other = local_gram(core, frames)
    tiles = (own + swapped(other)).reshape(64, 8, 128)
    parts = exchanged(tiles)
    held = chain(parts, rates)
    own = exchanged(held)
    begin = jnp.pad(start.T, ((0, 0), (0, 512 - start.shape[0])))
    other = swapped(own)
    own, other = own.reshape(512, 128), other.reshape(512, 128)
    return power_of(core, own, other, begin, clutter_cut, noise_cut, frames)


def solution(mesh):
    chips = Mesh(mesh.devices.reshape(4, 16, 2), ("tm", "chip", "core"))
    over = ("chip", "core")
    placed = (P("tm", None, over), P("tm", None), P(), P("tm"), P("tm"))
    return jax.shard_map(
        per_device, mesh=chips, in_specs=placed, out_specs=P("tm", over), check_vma=False
    )
```

```python
import functools

import jax
import jax.numpy as jnp
from jax import lax
from jax.experimental import pallas as pl
from jax.experimental.pallas import tpu as pltpu
from jax.sharding import Mesh, PartitionSpec as P


ITERS = 6
CHUNK = 2048
DEPTH = 3
COLS = 4096


def chunk_copy(frames_ref, kept_ref, sems, turn):
    span = pl.ds(pl.multiple_of(turn * CHUNK, CHUNK), CHUNK)
    return pltpu.make_async_copy(frames_ref.at[0, :, span], kept_ref.at[:, span], sems.at[turn])


def gram_kernel(chunks, frames_ref, packed_ref, kept_ref, left_ref, low_ref, sems):
    copy = functools.partial(chunk_copy, frames_ref, kept_ref, sems)

    for turn in range(DEPTH):
        copy(turn).start()
    left_ref[...] = jnp.zeros_like(left_ref)
    low_ref[...] = jnp.zeros_like(low_ref)
    rows = kept_ref.shape[0]
    rest = rows - 256

    def product(a, b):
        return lax.dot_general(a, b, (((1,), (1,)), ((), ())), preferred_element_type=jnp.float32)

    def one(turn, carry):
        copy(turn).wait()

        @pl.when(turn + DEPTH < chunks)
        def _():
            copy(turn + DEPTH).start()

        span = pl.ds(pl.multiple_of(turn * CHUNK, CHUNK), CHUNK)
        upper = kept_ref[0:256, span]
        lower = kept_ref[256:rows, span]
        left_ref[0:rows, :] += product(kept_ref[:, span], upper)
        low_ref[0:rest, 0:rest] += product(lower, lower)
        return carry

    lax.fori_loop(0, chunks, one, 0)
    down = lax.broadcasted_iota(jnp.int32, (256, 256), 0)
    across = lax.broadcasted_iota(jnp.int32, (256, 256), 1)
    low = low_ref[...]
    folded = jnp.where(down >= across, left_ref[0:256, :], low)
    diagonal = jnp.sum(jnp.where(down == across, low, 0.0), axis=0, keepdims=True)
    cross = jnp.where(down == 255, jnp.broadcast_to(diagonal, (256, 256)), left_ref[256:512, :])
    for spot, piece in ((0, folded), (32, cross)):
        for half in range(2):
            packed_ref[spot : spot + 32, half] = piece[:, 128 * half : 128 * (half + 1)].reshape(
                32, 8, 128
            )


def local_gram(frames):
    rows, columns = frames.shape[1:]
    chunks = columns // CHUNK
    return pl.pallas_call(
        functools.partial(gram_kernel, chunks),
        out_shape=jax.ShapeDtypeStruct((64, 2, 8, 128), jnp.float32),
        in_specs=[pl.BlockSpec(memory_space=pltpu.HBM)],
        out_specs=pl.BlockSpec(memory_space=pltpu.VMEM),
        scratch_shapes=[
            pltpu.VMEM((rows, columns), frames.dtype),
            pltpu.VMEM((512, 256), jnp.float32),
            pltpu.VMEM((256, 256), jnp.float32),
            pltpu.SemaphoreType.DMA((chunks,)),
        ],
        compiler_params=pltpu.CompilerParams(vmem_limit_bytes=56 * 2**20),
        cost_estimate=pl.CostEstimate(
            flops=2 * rows * rows * columns, bytes_accessed=2 * rows * columns, transcendentals=0
        ),
        name="local_gram",
    )(frames)


def chain_kernel(steps, group, copies, parts_ref, rates_ref, out_ref):
    held = None
    for step in range(steps):
        part = jnp.sum(parts_ref[step * group : (step + 1) * group], axis=0)
        held = part if step == 0 else rates_ref[step] * held + part
        out_ref[step * copies : (step + 1) * copies] = jnp.broadcast_to(
            held[None], (copies, 8, 128)
        )


def chain(parts, rates, copies):
    steps = rates.shape[0]
    return pl.pallas_call(
        functools.partial(chain_kernel, steps, parts.shape[0] // steps, copies),
        out_shape=jax.ShapeDtypeStruct((steps * copies, 8, 128), parts.dtype),
        compiler_params=pltpu.CompilerParams(vmem_limit_bytes=4 * 2**20),
        name="chain",
    )(parts, rates)


def split(x):
    high = x.astype(jnp.bfloat16)
    rest = x - high.astype(jnp.float32)
    middle = rest.astype(jnp.bfloat16)
    return high, middle, (rest - middle.astype(jnp.float32)).astype(jnp.bfloat16)


def mul(a, b, along=0):
    return lax.dot_general(
        a, b, (((1,), (along,)), ((), ())), preferred_element_type=jnp.float32
    )


def full_product(left, right, along=0):
    size = left[0].shape[0]
    stacked = jnp.concatenate(left, axis=0)
    first = mul(stacked, right[0], along)
    second = mul(stacked[: 2 * size], right[1], along)
    third = mul(left[0], right[2], along)
    small = first[2 * size :] + second[size:] + third
    return first[:size] + (first[size : 2 * size] + second[:size] + small)


def spread(x, index):
    return jnp.broadcast_to(x[index : index + 1, :], x.shape)


def eliminated(rows, none):
    rows = list(rows)
    count = len(rows)
    sub = lax.broadcasted_iota(jnp.int32, (8, 128), 0)

    def columns_of(v, first, size):
        return [
            jnp.broadcast_to(rows[v][:, first + k : first + k + 1], (8, 128))
            for k in range(size)
        ]

    done = []
    for a in range(0, count, 2):
        b = a + 1
        top = [column + none for column in columns_of(a, 8 * a, 8)]
        side = [column + none for column in columns_of(b, 8 * a, 8)]
        low = columns_of(b, 8 * b, 8)
        rest = {v: columns_of(v, 8 * a, 16) for v in range(b + 1, min(b + 3, count))}
        scales = []
        for half, own in ((0, top), (1, low)):
            pivots = jnp.ones((8, 128), jnp.float32)
            pivot = spread(own[0], 0)
            for j in range(8):
                pivots = jnp.where(sub == j, pivot, pivots)
                inverse = 1.0 / pivot
                heads = [spread(own[k], j) if k > j else None for k in range(8)]
                if j < 7:
                    pivot = spread(own[j + 1], j + 1) - (
                        spread(own[j], j + 1) * inverse
                    ) * heads[j + 1]
                lead = jnp.where(sub > j, own[j], 0.0) * inverse
                row = spread(rows[a + half], j)
                if half == 0:
                    beside = side[j] * inverse
                    others = [spread(side[j], k) for k in range(8)]
                    rows[b] = rows[b] - beside * row
                    for k in range(8):
                        low[k] = low[k] - beside * others[k]
                rows[a + half] = rows[a + half] - lead * row
                for k in range(j + 1, 8):
                    own[k] = own[k] - lead * heads[k]
                    if half == 0:
                        side[k] = side[k] - beside * heads[k]
                for v, held in rest.items():
                    far = held[8 * half + j] * inverse
                    for k in range(j + 1, 8):
                        held[8 * half + k] = held[8 * half + k] - far * heads[k]
                    if half == 0:
                        for k in range(8):
                            held[8 + k] = held[8 + k] - far * others[k]
                    rows[v] = rows[v] - far * row
            scales.append(1.0 / pivots)
            done.append(lax.rsqrt(pivots))
        if b + 3 < count:
            u1, u2, u3 = split(jnp.concatenate([rows[a], rows[b]], axis=0))
            t1, t2, t3 = split(
                jnp.concatenate([rows[a] * scales[0], rows[b] * scales[1]], axis=0)
            )
            change = lax.dot_general(
                jnp.concatenate([u1, u1, u2, u2, u1, u3], axis=0)[:, : 8 * count],
                jnp.concatenate([t1, t2, t1, t2, t3, t1], axis=0),
                (((0,), (0,)), ((), ())),
                preferred_element_type=jnp.float32,
            )
            for v in range(b + 3, count):
                rows[v] = rows[v] - change[8 * v : 8 * (v + 1), :]
    return [r * s for r, s in zip(rows, done)]


def power_kernel(
    chunks, core_ref, own_ref, other_ref, start_ref, low_ref, high_ref, frames_ref, out_ref,
    a1_ref, a2_ref, a3_ref, sized_ref, second_ref, kept_ref, zero_ref, sems,
):
    copy = functools.partial(chunk_copy, frames_ref, kept_ref, sems)
    for turn in range(chunks):
        copy(turn).start()
    zero_ref[...] = jnp.zeros_like(zero_ref)
    down = lax.broadcasted_iota(jnp.int32, (256, 256), 0)
    across = lax.broadcasted_iota(jnp.int32, (256, 256), 1)
    first = core_ref[0] == 0

    def whole(spot):
        own, other = own_ref[spot : spot + 256, :], other_ref[spot : spot + 256, :]
        return jnp.concatenate(
            [jnp.where(first, own, other), jnp.where(first, other, own)], axis=1
        )

    folded, cross = whole(0), whole(256)
    turned = folded.T
    top = jnp.where(down >= across, folded, turned)
    low = jnp.where(down < across, folded, turned)
    low = jnp.where(down == across, jnp.broadcast_to(cross[255:256, :], (256, 256)), low)
    cross = jnp.where(down == 255, 0.0, cross)

    def put(piece, i, j):
        for ref, part in zip((a1_ref, a2_ref, a3_ref), split(piece)):
            ref[256 * i : 256 * (i + 1), 256 * j : 256 * (j + 1)] = part

    put(top, 0, 0)
    put(low, 1, 1)
    put(cross, 1, 0)
    put(cross.T, 0, 1)

    rank, frames = start_ref.shape
    beside = lax.broadcasted_iota(jnp.int32, (rank, 128), 0) + rank
    unit = jnp.where(
        lax.broadcasted_iota(jnp.int32, (rank, 128), 1) == beside, 1.0, 0.0
    ).astype(jnp.float32)
    none = jnp.zeros((rank, frames), jnp.bfloat16)

    def under(parts):
        return [jnp.concatenate([none[:, : p.shape[1]], p], axis=0) for p in parts]

    def over(parts):
        return [jnp.concatenate([p, none[:, : p.shape[1]]], axis=0) for p in parts]

    def factor_of(gram):
        grown = gram + unit
        tiles = [grown[8 * v : 8 * (v + 1), :] for v in range(rank // 8)]
        return split(jnp.concatenate(eliminated(tiles, zero_ref[...]), axis=0))

    weights = (a1_ref, a2_ref, a3_ref)

    def iteration(turn, carry):
        product, gram = carry
        sized = split(full_product(factor_of(gram), under(split(product))))
        second = factor_of(full_product(sized, over(sized), 1))
        for at, part in enumerate(sized):
            sized_ref[at] = part
        for at, part in enumerate(second):
            second_ref[at] = part
        ahead = split(full_product(sized, [w[...] for w in weights]))
        square = split(full_product(ahead, under(ahead), 1))
        product = full_product(second, under(ahead))
        half = full_product(second, under(square))
        return product, full_product(split(half), over(second), 1)

    product = full_product(split(start_ref[...]), [w[...] for w in weights])
    parts = split(product)
    lax.fori_loop(0, ITERS, iteration, (product, full_product(parts, over(parts), 1)))
    subspace = full_product(
        [second_ref[at] for at in range(3)], under([sized_ref[at] for at in range(3)])
    )
    rows = kept_ref.shape[0]
    component = lax.broadcasted_iota(jnp.int32, subspace.shape, 0)
    band = (component >= low_ref[0]) & (component < high_ref[0])
    subspace_low = jnp.where(band, subspace, 0.0).astype(jnp.bfloat16)[:, :rows]

    def arrive(turn, carry):
        copy(turn).wait()
        return carry

    lax.fori_loop(0, chunks, arrive, 0)

    def project(turn, carry):
        span = pl.ds(pl.multiple_of(turn * COLS, COLS), COLS)
        values = mul(subspace_low, kept_ref[:, span])
        out_ref[:, span] = jnp.sum(values * values, axis=0, keepdims=True) / rows
        return carry

    lax.fori_loop(0, kept_ref.shape[1] // COLS, project, 0)


def power_of(core, own, other, start, low, high, frames):
    rows, columns = frames.shape[1:]
    chunks = columns // CHUNK
    return pl.pallas_call(
        functools.partial(power_kernel, chunks),
        out_shape=jax.ShapeDtypeStruct((1, columns), jnp.float32),
        in_specs=[
            pl.BlockSpec(memory_space=pltpu.SMEM),
            pl.BlockSpec(memory_space=pltpu.VMEM),
            pl.BlockSpec(memory_space=pltpu.VMEM),
            pl.BlockSpec(memory_space=pltpu.VMEM),
            pl.BlockSpec(memory_space=pltpu.SMEM),
            pl.BlockSpec(memory_space=pltpu.SMEM),
            pl.BlockSpec(memory_space=pltpu.HBM),
        ],
        out_specs=pl.BlockSpec(memory_space=pltpu.VMEM),
        scratch_shapes=[pltpu.VMEM((512, 512), jnp.bfloat16)] * 3
        + [
            pltpu.VMEM((3, 64, 512), jnp.bfloat16),
            pltpu.VMEM((3, 64, 128), jnp.bfloat16),
            pltpu.VMEM((rows, columns), frames.dtype),
            pltpu.VMEM((8, 128), jnp.float32),
            pltpu.SemaphoreType.DMA((chunks,)),
        ],
        compiler_params=pltpu.CompilerParams(vmem_limit_bytes=40 * 2**20),
        name="power",
    )(core, own, other, start, low, high, frames)


def tile_rates(decay):
    steps, group = lax.axis_size("tm"), lax.axis_size("chip")
    step = lax.axis_index("tm")
    turns = [decay] + [
        lax.ppermute(decay, "tm", [(i, (i + k) % steps) for i in range(steps)])
        for k in range(1, steps)
    ]
    every = []
    for t in range(steps):
        mine = jnp.zeros_like(decay)
        for k in range(steps):
            mine = mine + jnp.where((step - t) % steps == k, turns[k], 0.0)
        every.append(mine)
    rates = jnp.stack(every)
    rates = jnp.pad(rates, ((0, 0), (0, 512 - rates.shape[1])))
    first_row = 8 * (step * group + lax.axis_index("chip"))
    first_column = 128 * lax.axis_index("core")
    row = first_row + lax.broadcasted_iota(jnp.int32, (8, 128), 0)
    column = first_column + lax.broadcasted_iota(jnp.int32, (8, 128), 1)

    def at_rows(first):
        return lax.dynamic_slice_in_dim(rates, first, 8, 1)[:, :, None]

    def at_columns(first):
        return lax.dynamic_slice_in_dim(rates, first, 128, 1)[:, None, :]

    upper = at_rows(first_row) * at_columns(first_column)
    last = at_columns(256 + first_column)
    lower = at_rows(jnp.minimum(256 + first_row, 504)) * last
    return jnp.where(
        row == 511,
        last * last,
        jnp.where((row >= 256) | (row >= column), upper, lower),
    )


def swapped(x):
    return lax.ppermute(x, "core", [(0, 1), (1, 0)])


def exchanged(tiles, axes):
    return lax.all_to_all(tiles, axes, 0, 0, tiled=True)


def per_device(frames, decay, start, clutter_cut, noise_cut):
    core = lax.axis_index("core").reshape(1)
    rates = tile_rates(decay[0])
    packed = local_gram(frames)
    parts = exchanged(packed.reshape(128, 8, 128), ("tm", "chip", "core"))
    held = chain(parts, rates, lax.axis_size("chip"))
    own = exchanged(held, ("tm", "chip"))
    begin = jnp.pad(start.T, ((0, 0), (0, 512 - start.shape[0])))
    other = swapped(own)
    own, other = own.reshape(512, 128), other.reshape(512, 128)
    return power_of(core, own, other, begin, clutter_cut, noise_cut, frames)


def solution(mesh):
    chips = Mesh(mesh.devices.reshape(4, 16, 2), ("tm", "chip", "core"))
    over = ("chip", "core")
    placed = (P("tm", None, over), P("tm", None), P(), P("tm"), P("tm"))
    return jax.shard_map(
        per_device, mesh=chips, in_specs=placed, out_specs=P("tm", over), check_vma=False
    )
```

```python
import functools

import jax
import jax.numpy as jnp
from jax import lax
from jax.experimental import pallas as pl
from jax.experimental.pallas import tpu as pltpu
from jax.sharding import Mesh, PartitionSpec as P


ITERS = 6
CHUNK = 2048
COLS = 4096


def chunk_copy(frames_ref, kept_ref, sems, turn):
    span = pl.ds(pl.multiple_of(turn * CHUNK, CHUNK), CHUNK)
    return pltpu.make_async_copy(frames_ref.at[0, :, span], kept_ref.at[:, span], sems.at[turn])


def gram_kernel(chunks, frames_ref, packed_ref, kept_ref, left_ref, low_ref, sems):
    copy = functools.partial(chunk_copy, frames_ref, kept_ref, sems)

    for turn in range(chunks):
        copy(turn).start()
    left_ref[...] = jnp.zeros_like(left_ref)
    low_ref[...] = jnp.zeros_like(low_ref)
    rows = kept_ref.shape[0]
    rest = rows - 256

    def product(a, b):
        return lax.dot_general(a, b, (((1,), (1,)), ((), ())), preferred_element_type=jnp.float32)

    def one(turn, carry):
        copy(turn).wait()
        span = pl.ds(pl.multiple_of(turn * CHUNK, CHUNK), CHUNK)
        upper = kept_ref[0:256, span]
        lower = kept_ref[256:rows, span]
        left_ref[0:rows, :] += product(kept_ref[:, span], upper)
        low_ref[0:rest, 0:rest] += product(lower, lower)
        return carry

    lax.fori_loop(0, chunks, one, 0)
    down = lax.broadcasted_iota(jnp.int32, (256, 256), 0)
    across = lax.broadcasted_iota(jnp.int32, (256, 256), 1)
    low = low_ref[...]
    folded = jnp.where(down >= across, left_ref[0:256, :], low)
    diagonal = jnp.sum(jnp.where(down == across, low, 0.0), axis=0, keepdims=True)
    cross = jnp.where(down == 255, jnp.broadcast_to(diagonal, (256, 256)), left_ref[256:512, :])
    for spot, piece in ((0, folded), (32, cross)):
        for half in range(2):
            packed_ref[spot : spot + 32, half] = piece[:, 128 * half : 128 * (half + 1)].reshape(
                32, 8, 128
            )


def local_gram(frames):
    rows, columns = frames.shape[1:]
    chunks = columns // CHUNK
    return pl.pallas_call(
        functools.partial(gram_kernel, chunks),
        out_shape=pltpu.VMEM((64, 2, 8, 128), jnp.float32),
        in_specs=[pl.BlockSpec(memory_space=pltpu.HBM)],
        out_specs=pl.BlockSpec(memory_space=pltpu.VMEM),
        scratch_shapes=[
            pltpu.VMEM((rows, columns), frames.dtype),
            pltpu.VMEM((512, 256), jnp.float32),
            pltpu.VMEM((256, 256), jnp.float32),
            pltpu.SemaphoreType.DMA((chunks,)),
        ],
        compiler_params=pltpu.CompilerParams(vmem_limit_bytes=56 * 2**20),
        cost_estimate=pl.CostEstimate(
            flops=2 * rows * rows * columns, bytes_accessed=2 * rows * columns, transcendentals=0
        ),
        name="local_gram",
    )(frames)


def chain_kernel(steps, group, copies, parts_ref, rates_ref, out_ref):
    held = None
    for step in range(steps):
        part = jnp.sum(parts_ref[step * group : (step + 1) * group], axis=0)
        held = part if step == 0 else rates_ref[step] * held + part
        out_ref[step * copies : (step + 1) * copies] = jnp.broadcast_to(
            held[None], (copies, 8, 128)
        )


def chain(parts, rates, copies):
    steps = rates.shape[0]
    return pl.pallas_call(
        functools.partial(chain_kernel, steps, parts.shape[0] // steps, copies),
        out_shape=jax.ShapeDtypeStruct((steps * copies, 8, 128), parts.dtype),
        compiler_params=pltpu.CompilerParams(vmem_limit_bytes=4 * 2**20),
        name="chain",
    )(parts, rates)


def split(x):
    high = x.astype(jnp.bfloat16)
    rest = x - high.astype(jnp.float32)
    middle = rest.astype(jnp.bfloat16)
    return high, middle, (rest - middle.astype(jnp.float32)).astype(jnp.bfloat16)


def mul(a, b, along=0):
    return lax.dot_general(
        a, b, (((1,), (along,)), ((), ())), preferred_element_type=jnp.float32
    )


def full_product(left, right, along=0):
    size = left[0].shape[0]
    stacked = jnp.concatenate(left, axis=0)
    first = mul(stacked, right[0], along)
    second = mul(stacked[: 2 * size], right[1], along)
    third = mul(left[0], right[2], along)
    small = first[2 * size :] + second[size:] + third
    return first[:size] + (first[size : 2 * size] + second[:size] + small)


def spread(x, index):
    return jnp.broadcast_to(x[index : index + 1, :], x.shape)


def eliminated(rows, none, start):
    rows = list(rows)
    count = len(rows)
    sub = lax.broadcasted_iota(jnp.int32, (8, 128), 0)

    def columns_of(v, first, size):
        return [
            jnp.broadcast_to(rows[v][:, start + first + k : start + first + k + 1], (8, 128))
            for k in range(size)
        ]

    done = []
    for a in range(0, count, 2):
        b = a + 1
        top = [column + none for column in columns_of(a, 8 * a, 8)]
        side = [column + none for column in columns_of(b, 8 * a, 8)]
        low = columns_of(b, 8 * b, 8)
        rest = {v: columns_of(v, 8 * a, 16) for v in range(b + 1, min(b + 3, count))}
        scales = []
        for half, own in ((0, top), (1, low)):
            pivots = jnp.ones((8, 128), jnp.float32)
            pivot = spread(own[0], 0)
            for j in range(8):
                pivots = jnp.where(sub == j, pivot, pivots)
                inverse = 1.0 / pivot
                heads = [spread(own[k], j) if k > j else None for k in range(8)]
                if j < 7:
                    pivot = spread(own[j + 1], j + 1) - (
                        spread(own[j], j + 1) * inverse
                    ) * heads[j + 1]
                lead = jnp.where(sub > j, own[j], 0.0) * inverse
                row = spread(rows[a + half], j)
                if half == 0:
                    beside = side[j] * inverse
                    others = [spread(side[j], k) for k in range(8)]
                    rows[b] = rows[b] - beside * row
                    for k in range(8):
                        low[k] = low[k] - beside * others[k]
                rows[a + half] = rows[a + half] - lead * row
                for k in range(j + 1, 8):
                    own[k] = own[k] - lead * heads[k]
                    if half == 0:
                        side[k] = side[k] - beside * heads[k]
                for v, held in rest.items():
                    far = held[8 * half + j] * inverse
                    for k in range(j + 1, 8):
                        held[8 * half + k] = held[8 * half + k] - far * heads[k]
                    if half == 0:
                        for k in range(8):
                            held[8 + k] = held[8 + k] - far * others[k]
                    rows[v] = rows[v] - far * row
            scales.append(1.0 / pivots)
            done.append(lax.rsqrt(pivots))
        if b + 3 < count:
            u1, u2, u3 = split(jnp.concatenate([rows[a], rows[b]], axis=0))
            t1, t2, t3 = split(
                jnp.concatenate([rows[a] * scales[0], rows[b] * scales[1]], axis=0)
            )
            change = lax.dot_general(
                jnp.concatenate([u1, u1, u2, u2, u1, u3], axis=0)[:, : start + 8 * count],
                jnp.concatenate([t1, t2, t1, t2, t3, t1], axis=0),
                (((0,), (0,)), ((), ())),
                preferred_element_type=jnp.float32,
            )
            for v in range(b + 3, count):
                rows[v] = rows[v] - change[start + 8 * v : start + 8 * (v + 1), :]
    return [r * s for r, s in zip(rows, done)]


def power_kernel(
    chunks, core_ref, own_ref, other_ref, start_ref, low_ref, high_ref, frames_ref, out_ref,
    a1_ref, a2_ref, a3_ref, kept_ref, zero_ref, sems,
):
    copy = functools.partial(chunk_copy, frames_ref, kept_ref, sems)
    for turn in range(chunks):
        copy(turn).start()
    zero_ref[...] = jnp.zeros_like(zero_ref)
    down = lax.broadcasted_iota(jnp.int32, (256, 256), 0)
    across = lax.broadcasted_iota(jnp.int32, (256, 256), 1)
    first = core_ref[0] == 0

    def whole(spot):
        own, other = own_ref[spot : spot + 256, :], other_ref[spot : spot + 256, :]
        return jnp.concatenate(
            [jnp.where(first, own, other), jnp.where(first, other, own)], axis=1
        )

    folded, cross = whole(0), whole(256)
    turned = folded.T
    top = jnp.where(down >= across, folded, turned)
    low = jnp.where(down < across, folded, turned)
    low = jnp.where(down == across, jnp.broadcast_to(cross[255:256, :], (256, 256)), low)
    cross = jnp.where(down == 255, 0.0, cross)

    def put(piece, i, j):
        for ref, part in zip((a1_ref, a2_ref, a3_ref), split(piece)):
            ref[256 * i : 256 * (i + 1), 256 * j : 256 * (j + 1)] = part

    put(top, 0, 0)
    put(low, 1, 1)
    put(cross, 1, 0)
    put(cross.T, 0, 1)

    rank, frames = start_ref.shape
    line = lax.broadcasted_iota(jnp.int32, (rank, 128), 0)
    lane = lax.broadcasted_iota(jnp.int32, (rank, 128), 1)
    none = jnp.zeros((rank, frames), jnp.bfloat16)

    def under(parts):
        return [jnp.concatenate([none[:, : p.shape[1]], p], axis=0) for p in parts]

    def over(parts):
        return [jnp.concatenate([p, none[:, : p.shape[1]]], axis=0) for p in parts]

    def factor_of(gram, start=0):
        grown = jnp.where(lane == line + (rank - start), 1.0, gram)
        tiles = [grown[8 * v : 8 * (v + 1), :] for v in range(rank // 8)]
        return jnp.concatenate(eliminated(tiles, zero_ref[...], start), axis=0)

    weights = (a1_ref, a2_ref, a3_ref)

    def iteration(turn, subspace):
        sized = split(subspace)
        ahead = split(full_product(sized, [w[...] for w in weights]))
        square = full_product(ahead, under(ahead), 1)
        gram = full_product(sized, over(sized), 1)
        first = factor_of(square, rank)
        second = factor_of(jnp.where(turn > 0, gram, jnp.where(lane == line, 1.0, 0.0)))
        product = full_product(split(second), under(ahead))
        turned = split(jnp.where((lane < rank) & (lane >= line), second, 0.0))
        both = full_product(split(first), over(turned), 1)
        return full_product(split(both), over(split(product)))

    subspace = lax.fori_loop(0, ITERS, iteration, start_ref[...])
    sized = split(subspace)
    gram = full_product(sized, over(sized), 1)
    subspace = full_product(split(factor_of(gram)), under(sized))
    rows = kept_ref.shape[0]
    component = lax.broadcasted_iota(jnp.int32, subspace.shape, 0)
    band = (component >= low_ref[0]) & (component < high_ref[0])
    subspace_low = jnp.where(band, subspace, 0.0).astype(jnp.bfloat16)[:, :rows]

    def arrive(turn, carry):
        copy(turn).wait()
        return carry

    lax.fori_loop(0, chunks, arrive, 0)

    def project(turn, carry):
        span = pl.ds(pl.multiple_of(turn * COLS, COLS), COLS)
        values = mul(subspace_low, kept_ref[:, span])
        out_ref[:, span] = jnp.sum(values * values, axis=0, keepdims=True) / rows
        return carry

    lax.fori_loop(0, kept_ref.shape[1] // COLS, project, 0)


def power_of(core, own, other, start, low, high, frames):
    rows, columns = frames.shape[1:]
    chunks = columns // CHUNK
    return pl.pallas_call(
        functools.partial(power_kernel, chunks),
        out_shape=jax.ShapeDtypeStruct((1, columns), jnp.float32),
        in_specs=[
            pl.BlockSpec(memory_space=pltpu.SMEM),
            pl.BlockSpec(memory_space=pltpu.VMEM),
            pl.BlockSpec(memory_space=pltpu.VMEM),
            pl.BlockSpec(memory_space=pltpu.VMEM),
            pl.BlockSpec(memory_space=pltpu.SMEM),
            pl.BlockSpec(memory_space=pltpu.SMEM),
            pl.BlockSpec(memory_space=pltpu.HBM),
        ],
        out_specs=pl.BlockSpec(memory_space=pltpu.VMEM),
        scratch_shapes=[pltpu.VMEM((512, 512), jnp.bfloat16)] * 3
        + [
            pltpu.VMEM((rows, columns), frames.dtype),
            pltpu.VMEM((8, 128), jnp.float32),
            pltpu.SemaphoreType.DMA((chunks,)),
        ],
        compiler_params=pltpu.CompilerParams(vmem_limit_bytes=40 * 2**20),
        name="power",
    )(core, own, other, start, low, high, frames)


def tile_rates(decay):
    steps, group = lax.axis_size("tm"), lax.axis_size("chip")
    step = lax.axis_index("tm")
    turns = [decay] + [
        lax.ppermute(decay, "tm", [(i, (i + k) % steps) for i in range(steps)])
        for k in range(1, steps)
    ]
    every = []
    for t in range(steps):
        mine = jnp.zeros_like(decay)
        for k in range(steps):
            mine = mine + jnp.where((step - t) % steps == k, turns[k], 0.0)
        every.append(mine)
    rates = jnp.stack(every)
    rates = jnp.pad(rates, ((0, 0), (0, 512 - rates.shape[1])))
    first_row = 8 * (step * group + lax.axis_index("chip"))
    first_column = 128 * lax.axis_index("core")
    row = first_row + lax.broadcasted_iota(jnp.int32, (8, 128), 0)
    column = first_column + lax.broadcasted_iota(jnp.int32, (8, 128), 1)

    def at_rows(first):
        return lax.dynamic_slice_in_dim(rates, first, 8, 1)[:, :, None]

    def at_columns(first):
        return lax.dynamic_slice_in_dim(rates, first, 128, 1)[:, None, :]

    upper = at_rows(first_row) * at_columns(first_column)
    last = at_columns(256 + first_column)
    lower = at_rows(jnp.minimum(256 + first_row, 504)) * last
    return jnp.where(
        row == 511,
        last * last,
        jnp.where((row >= 256) | (row >= column), upper, lower),
    )


def swapped(x):
    return lax.ppermute(x, "core", [(0, 1), (1, 0)])


def exchanged(tiles, axes):
    return lax.all_to_all(tiles, axes, 0, 0, tiled=True)


def per_device(frames, decay, start, clutter_cut, noise_cut):
    core = lax.axis_index("core").reshape(1)
    rates = tile_rates(decay[0])
    packed = local_gram(frames)
    parts = exchanged(packed.reshape(128, 8, 128), ("tm", "chip", "core"))
    held = chain(parts, rates, lax.axis_size("chip"))
    own = exchanged(held, ("tm", "chip"))
    begin = jnp.pad(start.T, ((0, 0), (0, 512 - start.shape[0])))
    other = swapped(own)
    own, other = own.reshape(512, 128), other.reshape(512, 128)
    return power_of(core, own, other, begin, clutter_cut, noise_cut, frames)


def solution(mesh):
    chips = Mesh(mesh.devices.reshape(4, 16, 2), ("tm", "chip", "core"))
    over = ("chip", "core")
    placed = (P("tm", None, over), P("tm", None), P(), P("tm"), P("tm"))
    return jax.shard_map(
        per_device, mesh=chips, in_specs=placed, out_specs=P("tm", over), check_vma=False
    )
```
